32 devices in a mesh: row: 8 (over z, y), col: 4 (over x, core).
Axes of the slice: x: 2, y: 2, z: 4, core: 2. Of those that a mesh axis runs over, the one named last changes fastest.
Arguments:
- t2_amps: bfloat16 [2048, 1024], P('row', 'col'), may hold values from -6 to 6
- v_ints: bfloat16 [1024, 8192], P('row', 'col'), may hold values from -0.375 to 0.375
- t2_mask: int32 [16, 8], P('row', 'col'), may hold values from 0 to 1, as said below
- v_mask: int32 [8, 64], P('row', 'col'), may hold values from 0 to 1, as said below
Outputs:
- ladder: bfloat16 [2048, 8192], P('row', 'col')
The draws below stay inside these ranges and needn't reach their ends.
Inputs may be any that keep to these rules, and one draw needn't show every extreme that they name: t2_mask[i, k] is 1 exactly where the symmetry sector of occupied-pair tile i equals that of contraction tile k, else 0; the sectors are 0 to 3, and each of the four labels at least one occupied-pair tile and at least one contraction tile. v_mask[k, n] is 1 exactly where the sector of contraction tile k (the same labels as in t2_mask) equals that of column tile n, else 0; the column tiles fall into aligned blocks of 16, one block for each col index, and in every block one sector labels exactly 8 tiles and no sector labels more than 8.
All inputs are finite; a program needn't handle non-finite values.
Results may differ from the reference program's by a relative error of at most 0.001.
Values may be sent and summed in bfloat16 or wider, within the bound.
A program may use at most 64 MiB of HBM per device.

```python
import jax
import jax.numpy as jnp

TILE = 128
NT_DEV = 16
MR = 16
NC = 64
KT = 8
CAP = 8


def shuffled_labels(key, labels):
    count = labels.shape[0]
    places = jnp.arange(count, dtype=jnp.int32)
    forced = jnp.where(places < 4, places, labels).astype(jnp.int32)
    return jax.random.permutation(key, forced)


def sector_labels(key):
    k_raw = jax.random.randint(jax.random.fold_in(key, 11), (KT,), 0, 20)
    k_first = (k_raw >= 10).astype(jnp.int32) + (k_raw >= 15).astype(jnp.int32) + (k_raw >= 18).astype(jnp.int32)
    k_sector = shuffled_labels(jax.random.fold_in(key, 21), k_first)
    row_raw = jax.random.randint(jax.random.fold_in(key, 12), (MR,), 0, 8)
    row_first = jnp.minimum(row_raw, 3).astype(jnp.int32)
    row_sector = shuffled_labels(jax.random.fold_in(key, 22), row_first)
    block_count = NC // NT_DEV
    dominant = jax.random.randint(jax.random.fold_in(key, 13), (block_count,), 0, 4)
    offsets = jax.random.randint(jax.random.fold_in(key, 14), (block_count, NT_DEV), 0, 3)
    others = (dominant[:, None] + 1 + offsets) % 4
    places = jnp.arange(NT_DEV, dtype=jnp.int32)
    unshuffled = jnp.where(places[None, :] < CAP, dominant[:, None], others).astype(jnp.int32)
    block_keys = jax.random.split(jax.random.fold_in(key, 15), block_count)
    shuffled = jax.vmap(lambda one_key, labels: jax.random.permutation(one_key, labels))(block_keys, unshuffled)
    col_sector = shuffled.reshape(-1).astype(jnp.int32)
    return (row_sector, k_sector, col_sector)


def draw_t2_mask(key, part):
    row_sector, k_sector, col_sector = sector_labels(key)
    return (row_sector[:, None] == k_sector[None, :]).astype(jnp.int32)


def draw_v_mask(key, part):
    row_sector, k_sector, col_sector = sector_labels(key)
    return (k_sector[:, None] == col_sector[None, :]).astype(jnp.int32)


def block_levels(rng, extent, cuts, low, top_value):
    gain, own = 1.0, jax.random.fold_in(rng, 6)
    for axis_at, parts in cuts:
        heights = jnp.exp(jax.random.uniform(jax.random.fold_in(own, axis_at), (parts,), jnp.float32, low / len(cuts), top_value / len(cuts)))
        gain = gain * jnp.repeat(heights, extent[axis_at] // parts).reshape([-1 if axis == axis_at else 1 for axis in range(len(extent))])
    return gain


def normal_values(own_key, shape, scale, most, cuts=(), held_as=jnp.bfloat16):
    drawn = scale * jax.random.normal(own_key, shape, jnp.float32)
    if cuts:
        drawn = drawn * block_levels(own_key, shape, cuts, -0.22, 0.18)
    return jnp.clip(drawn, -most, most).astype(held_as)


def setup_inputs(seed: int = 0) -> dict:
    seeds = jax.random.split(jax.random.key(seed), 5)
    return {
        "t2_amps": normal_values(seeds[0], (MR * TILE, KT * TILE), 1.0, 6.0, ((0, 8), (1, 4))),
        "v_ints": normal_values(seeds[1], (KT * TILE, NC * TILE), (KT * TILE // 4) ** -0.5, 0.375, ((0, 8), (1, 4))),
        "t2_mask": draw_t2_mask(jax.random.fold_in(seeds[4], 71), 0),
        "v_mask": draw_v_mask(jax.random.fold_in(seeds[4], 71), 0),
    }


def expand_mask(mask, tile):
    wide = jnp.repeat(jnp.repeat(mask, tile, axis=0), tile, axis=1)
    return wide.astype(jnp.bfloat16)


def reference(t2_amps, v_ints, t2_mask, v_mask):
    t2_sparse = t2_amps * expand_mask(t2_mask, TILE)
    v_sparse = v_ints * expand_mask(v_mask, TILE)
    ladder = jnp.dot(t2_sparse, v_sparse, preferred_element_type=jnp.float32)
    return ladder.astype(jnp.bfloat16)
```

```python
import functools

import jax
import jax.numpy as jnp
from jax import lax
from jax.experimental import pallas as pl
from jax.experimental.pallas import tpu as pltpu
from jax.sharding import PartitionSpec as P

MESH = pl.DeviceIdType.MESH


def grid_of(mesh):
    rows = mesh.shape["row"]
    ny = 1
    while 2 * (2 * ny) * (2 * ny) <= rows:
        ny *= 2
    return (rows // ny, ny) if rows % ny == 0 else (rows, 1)


def signs(d):
    return (0,) if d == 0 else (d, -d)


def gather_kernel(nz, ny, nc, tm_ref, vm_ref, t_ref, v_ref, o_ref, p_ref,
                  tbuf, vbuf, posbuf, acc, t_send, t_recv, send, recv):
    me, col = lax.axis_index("row"), lax.axis_index("col")
    z, y = me // ny, me % ny
    mr, kpc = tm_ref.shape
    nt = vm_ref.shape[1]
    tile = v_ref.shape[0]
    rows = t_ref.shape[0]
    cap = nt // 2
    nr = nz * ny
    f32 = jnp.float32

    dirs = ((1, 0), (-1, 0), (0, 1), (0, -1))

    def inside(dz, dy):
        ok = jnp.bool_(True)
        if dz > 0:
            ok = ok & (z + dz < nz)
        if dz < 0:
            ok = ok & (z + dz >= 0)
        if dy > 0:
            ok = ok & (y + dy < ny)
        if dy < 0:
            ok = ok & (y + dy >= 0)
        return ok

    live = [d for d in range(4) if (nz > 1 if d < 2 else ny > 1)]

    barrier = pltpu.get_barrier_semaphore()
    expect = jnp.int32(nc - 1)
    for d in live:
        dz, dy = dirs[d]
        ok = inside(dz, dy)
        expect = expect + ok.astype(jnp.int32)

        @pl.when(ok)
        def _():
            pl.semaphore_signal(barrier, inc=1, device_id=(me + dz * ny + dy, col), device_id_type=MESH)

    for s in range(1, nc):
        pl.semaphore_signal(barrier, inc=1, device_id=(me, lax.rem(col + s, nc)), device_id_type=MESH)

    bf16 = jnp.bfloat16
    count, slots = jnp.int32(0), []
    for n in range(nt):
        m = vm_ref[0, n]
        slots.append(jnp.broadcast_to((m * (count + 1)).astype(f32), (16, tile)))
        count = count + m

    def down(x):
        return jnp.broadcast_to(x.astype(bf16)[None], (tile // 16, 16, tile)).reshape(tile, tile)

    for j in range(cap):
        total = None
        for n in range(j, nt):
            hit = down(jnp.maximum(1.0 - jnp.abs(slots[n] - (j + 1.0)), 0.0))
            term = v_ref[:, n * tile:(n + 1) * tile] * hit
            total = term if total is None else total + term
        vbuf[me, :, j * tile:(j + 1) * tile] = total
    lane = lax.broadcasted_iota(jnp.int32, posbuf.shape[1:], 1)
    place = jnp.zeros(posbuf.shape[1:], f32)
    for n in range(nt):
        place = jnp.where(lane == n, slots[n][:8], place)
    posbuf[me] = place
    for i in range(mr):
        for k in range(kpc):
            part = t_ref[i * tile:(i + 1) * tile, k * tile:(k + 1) * tile]
            flag = down(jnp.broadcast_to(tm_ref[i, k].astype(f32), (16, tile)))
            tbuf[col, i * tile:(i + 1) * tile, k * tile:(k + 1) * tile] = part * flag
    row16 = lax.broadcasted_iota(jnp.int32, (tbuf.shape[1] - rows, tile), 0)
    for k in range(kpc):
        flags = jnp.zeros(row16.shape, f32)
        for i in range(mr):
            flags = jnp.where(row16 == i, tm_ref[i, k].astype(f32), flags)
        tbuf[col, rows:, k * tile:(k + 1) * tile] = flags.astype(tbuf.dtype)

    pl.semaphore_wait(barrier, expect)

    head = tile // 8
    cuts = [(0, head), (head, 3 * head), (4 * head, 2 * head), (6 * head, 2 * head)]
    small = len(cuts)

    def piece(src, c):
        if c == small:
            return posbuf.at[src]
        return vbuf.at[src, pl.ds(cuts[c][0], cuts[c][1])]

    def copy(src, c, d):
        dz, dy = dirs[d]
        return pltpu.make_async_remote_copy(
            src_ref=piece(src, c), dst_ref=piece(src, c),
            send_sem=send.at[d, src, c], recv_sem=recv.at[src, c],
            device_id=(me + dz * ny + dy, col), device_id_type=MESH)

    sent = []

    def forward(src, c, d, valid):
        dz, dy = dirs[d]
        ok = inside(dz, dy) if valid is None else valid & inside(dz, dy)

        @pl.when(ok)
        def _():
            copy(src, c, d).start()

        sent.append((src, c, d, ok))

    def arrive(src, c):
        pltpu.make_async_remote_copy(
            src_ref=piece(src, c), dst_ref=piece(src, c),
            send_sem=send.at[0, src, c], recv_sem=recv.at[src, c],
            device_id=(me, col), device_id_type=MESH).wait_recv()

    def step_dirs(a, b, first):
        zdir = [0] if a > 0 else [1] if a < 0 else [0, 1]
        ydir = [2] if b > 0 else [3] if b < 0 else [2, 3]
        if first:
            out = zdir + (ydir if a == 0 else [])
        else:
            out = (zdir if b == 0 else []) + ydir
        keep = []
        for d in out:
            if d not in live:
                continue
            if d < 2 and abs(a + dirs[d][0]) >= nz:
                continue
            if d >= 2 and abs(b + dirs[d][1]) >= ny:
                continue
            keep.append(d)
        return keep

    heads = [0, small]
    bodies = list(range(1, small))

    for c in [0, small] + bodies:
        for d in live:
            forward(me, c, d, None)

    t_copies = []
    for s in range(1, nc):
        t_copies.append(pltpu.make_async_remote_copy(
            src_ref=tbuf.at[col], dst_ref=tbuf.at[col],
            send_sem=t_send.at[s], recv_sem=t_recv.at[s],
            device_id=(me, lax.rem(col + s, nc)), device_id_type=MESH))
        t_copies[-1].start()

    def event(a, b, cs, first):
        valid = inside(-a, -b)
        src = me - a * ny - b
        for c in cs:
            @pl.when(valid)
            def _():
                arrive(src, c)

            for d in step_dirs(a, b, first):
                forward(src, c, d, valid)

    for key in range(1, nz + ny - 1):
        for db in range(min(key, ny - 1), -1, -1):
            da = key - db
            if da >= nz:
                continue
            for a in signs(da):
                for b in signs(db):
                    event(a, b, heads, True)
        for db in range(0, ny - 1):
            da = key - db
            if da >= nz or da < 0:
                continue
            for c in bodies:
                for a in signs(da):
                    for b in signs(db):
                        event(a, b, [c], False)

    for t in t_copies:
        t.wait()

    acc[...] = jnp.zeros_like(acc)
    wide = 2 * tile

    def multiply(src):
        left = tbuf[src // kpc, :rows, pl.ds(pl.multiple_of(lax.rem(src, kpc) * tile, tile), tile)]
        for n in range(0, cap * tile, wide):
            acc[:, n:n + wide] += jnp.dot(left, vbuf[src, :, n:n + wide], preferred_element_type=f32)

    def local(zz, carry):
        for yy in range(ny):
            pass
        multiply(zz * ny + y)
        return carry

    lax.fori_loop(0, nz, local, 0)

    for src, c, d, ok in sent[:len(sent) // 2]:
        @pl.when(ok)
        def _():
            copy(src, c, d).wait_send()

    far = [b for b in range(-(ny - 1), ny) if b != 0]

    def across(s, carry):
        dist = (s + 1) // 2
        a = jnp.where(s % 2 == 1, dist, -dist)
        zz = z - a
        for b in far:
            ok = (zz >= 0) & (zz < nz) & (y - b >= 0) & (y - b < ny)
            src = zz * ny + y - b

            @pl.when(ok)
            def _():
                if abs(b) == ny - 1:
                    for c in bodies:
                        arrive(src, c)
                multiply(src)
        return carry

    lax.fori_loop(0, 2 * nz - 1, across, 0)

    for src, c, d, ok in sent[len(sent) // 2:]:
        @pl.when(ok)
        def _():
            copy(src, c, d).wait_send()

    o_ref[...] = acc[...].astype(o_ref.dtype)

    p_ref[...] = jnp.zeros_like(p_ref)
    for i in range(mr):
        best = jnp.zeros((1, posbuf.shape[2]), f32)
        for src in range(nr):
            kk = (src % kpc) * tile
            flag = tbuf[src // kpc, rows:, kk:kk + tile].astype(f32)[i:i + 1]
            best = jnp.maximum(best, flag * posbuf[src, 0:1, :])
        p_ref[i:i + 1, :] = best.astype(jnp.int32)


def spread_kernel(per, p_ref, o_ref, out_ref):
    tile = out_ref.shape[1] // per
    for i in range(out_ref.shape[0] // tile):
        here = slice(i * tile, (i + 1) * tile)
        for q in range(per):
            slot = p_ref[i, pl.program_id(0) * per + q]
            at = pl.multiple_of(jnp.maximum(slot - 1, 0) * tile, tile)
            got = o_ref[here, pl.ds(at, tile)]
            out_ref[here, q * tile:(q + 1) * tile] = jnp.where(slot > 0, got, jnp.zeros_like(got))


def solution(mesh):
    nz, ny = grid_of(mesh)
    nc = mesh.shape["col"]

    def on_device(t2_amps, v_ints, t2_mask, v_mask):
        rows, kcols = t2_amps.shape
        tile, ncols = v_ints.shape
        mr = t2_mask.shape[0]
        nt = v_mask.shape[1]
        cap = nt // 2
        nr = nz * ny
        pieces = 5
        vmem = pl.BlockSpec(memory_space=pltpu.VMEM)
        smem = pl.BlockSpec(memory_space=pltpu.SMEM)
        dense, places = pl.pallas_call(
            functools.partial(gather_kernel, nz, ny, nc),
            name="gather",
            out_shape=(jax.ShapeDtypeStruct((rows, cap * tile), jnp.bfloat16),
                       jax.ShapeDtypeStruct((8, 128), jnp.int32)),
            in_specs=[smem, smem, vmem, vmem],
            out_specs=(vmem, vmem),
            scratch_shapes=[
                pltpu.VMEM((nc, rows + 16, kcols), jnp.bfloat16),
                pltpu.VMEM((nr, tile, cap * tile), jnp.bfloat16),
                pltpu.VMEM((nr, 8, 128), jnp.float32),
                pltpu.VMEM((rows, cap * tile), jnp.float32),
                pltpu.SemaphoreType.DMA((nc,)),
                pltpu.SemaphoreType.DMA((nc,)),
                pltpu.SemaphoreType.DMA((4, nr, pieces)),
                pltpu.SemaphoreType.DMA((nr, pieces)),
            ],
            compiler_params=pltpu.CompilerParams(collective_id=0, has_side_effects=True),
        )(t2_mask, v_mask, t2_amps, v_ints)
        per = max(nt // 4, 1)
        return pl.pallas_call(
            functools.partial(spread_kernel, per),
            name="spread",
            grid=(nt // per,),
            out_shape=jax.ShapeDtypeStruct((rows, ncols), jnp.bfloat16),
            in_specs=[smem, pl.BlockSpec((rows, cap * tile), lambda n: (0, 0))],
            out_specs=pl.BlockSpec((rows, per * tile), lambda n: (0, n)),
        )(places, dense)

    return jax.shard_map(
        on_device,
        mesh=mesh,
        in_specs=(P("row", "col"), P("row", "col"), P("row", "col"), P("row", "col")),
        out_specs=P("row", "col"),
        check_vma=False,
    )
```

```python
import functools

import jax
import jax.numpy as jnp
from jax import lax
from jax.experimental import pallas as pl
from jax.experimental.pallas import tpu as pltpu
from jax.sharding import PartitionSpec as P

MESH = pl.DeviceIdType.MESH


def grid_of(mesh):
    rows = mesh.shape["row"]
    ny = 1
    while 2 * (2 * ny) * (2 * ny) <= rows:
        ny *= 2
    return (rows // ny, ny) if rows % ny == 0 else (rows, 1)


def signs(d):
    return (0,) if d == 0 else (d, -d)


def gather_kernel(nz, ny, nc, tm_ref, vm_ref, t_hbm, v_hbm, o_ref, p_ref,
                  t_ref, v_ref, load, tbuf, vbuf, posbuf, acc, t_send, t_recv, send, recv):
    me, col = lax.axis_index("row"), lax.axis_index("col")
    z, y = me // ny, me % ny
    mr, kpc = tm_ref.shape
    nt = vm_ref.shape[1]
    tile = v_ref.shape[0]
    rows = t_ref.shape[0]
    cap = nt // 2
    nr = nz * ny
    f32 = jnp.float32

    dirs = ((1, 0), (-1, 0), (0, 1), (0, -1))

    def inside(dz, dy):
        ok = jnp.bool_(True)
        if dz > 0:
            ok = ok & (z + dz < nz)
        if dz < 0:
            ok = ok & (z + dz >= 0)
        if dy > 0:
            ok = ok & (y + dy < ny)
        if dy < 0:
            ok = ok & (y + dy >= 0)
        return ok

    live = [d for d in range(4) if (nz > 1 if d < 2 else ny > 1)]

    barrier = pltpu.get_barrier_semaphore()
    expect = jnp.int32(nc - 1)
    for d in live:
        dz, dy = dirs[d]
        ok = inside(dz, dy)
        expect = expect + ok.astype(jnp.int32)

        @pl.when(ok)
        def _():
            pl.semaphore_signal(barrier, inc=1, device_id=(me + dz * ny + dy, col), device_id_type=MESH)

    for s in range(1, nc):
        pl.semaphore_signal(barrier, inc=1, device_id=(me, lax.rem(col + s, nc)), device_id_type=MESH)

    loads = [pltpu.make_async_copy(v_hbm, v_ref, load.at[0]), pltpu.make_async_copy(t_hbm, t_ref, load.at[1])]
    for one in loads:
        one.start()

    bf16 = jnp.bfloat16
    count, slots = jnp.int32(0), []
    for n in range(nt):
        m = vm_ref[0, n]
        slots.append(jnp.broadcast_to((m * (count + 1)).astype(f32), (16, tile)))
        count = count + m

    def down(x):
        return jnp.broadcast_to(x.astype(bf16)[None], (tile // 16, 16, tile)).reshape(tile, tile)

    for one in loads:
        one.wait()
    for j in range(cap):
        total = None
        for n in range(j, nt):
            hit = down(jnp.maximum(1.0 - jnp.abs(slots[n] - (j + 1.0)), 0.0))
            term = v_ref[:, n * tile:(n + 1) * tile] * hit
            total = term if total is None else total + term
        vbuf[me, :, j * tile:(j + 1) * tile] = total
    lane = lax.broadcasted_iota(jnp.int32, posbuf.shape[1:], 1)
    place = jnp.zeros(posbuf.shape[1:], f32)
    for n in range(nt):
        place = jnp.where(lane == n, slots[n][:8], place)
    posbuf[me] = place
    for i in range(mr):
        for k in range(kpc):
            part = t_ref[i * tile:(i + 1) * tile, k * tile:(k + 1) * tile]
            flag = down(jnp.broadcast_to(tm_ref[i, k].astype(f32), (16, tile)))
            tbuf[col, i * tile:(i + 1) * tile, k * tile:(k + 1) * tile] = part * flag
    row16 = lax.broadcasted_iota(jnp.int32, (tbuf.shape[1] - rows, tile), 0)
    for k in range(kpc):
        flags = jnp.zeros(row16.shape, f32)
        for i in range(mr):
            flags = jnp.where(row16 == i, tm_ref[i, k].astype(f32), flags)
        tbuf[col, rows:, k * tile:(k + 1) * tile] = flags.astype(tbuf.dtype)

    pl.semaphore_wait(barrier, expect)

    head = tile // 8
    cuts = [(0, head), (head, 2 * head), (3 * head, 2 * head), (5 * head, 2 * head), (7 * head, head)]
    small = len(cuts)

    def piece(src, c):
        if c == small:
            return posbuf.at[src]
        return vbuf.at[src, pl.ds(cuts[c][0], cuts[c][1])]

    def copy(src, c, d):
        dz, dy = dirs[d]
        return pltpu.make_async_remote_copy(
            src_ref=piece(src, c), dst_ref=piece(src, c),
            send_sem=send.at[d, src, c], recv_sem=recv.at[src, c],
            device_id=(me + dz * ny + dy, col), device_id_type=MESH)

    sent = []

    def forward(src, c, d, valid):
        dz, dy = dirs[d]
        ok = inside(dz, dy) if valid is None else valid & inside(dz, dy)

        @pl.when(ok)
        def _():
            copy(src, c, d).start()

        sent.append((src, c, d, ok))

    def arrive(src, c):
        pltpu.make_async_remote_copy(
            src_ref=piece(src, c), dst_ref=piece(src, c),
            send_sem=send.at[0, src, c], recv_sem=recv.at[src, c],
            device_id=(me, col), device_id_type=MESH).wait_recv()

    def step_dirs(a, b, first):
        zdir = [0] if a > 0 else [1] if a < 0 else [0, 1]
        ydir = [2] if b > 0 else [3] if b < 0 else [2, 3]
        if first:
            out = zdir + (ydir if a == 0 else [])
        else:
            out = (zdir if b == 0 else []) + ydir
        keep = []
        for d in out:
            if d not in live:
                continue
            if d < 2 and abs(a + dirs[d][0]) >= nz:
                continue
            if d >= 2 and abs(b + dirs[d][1]) >= ny:
                continue
            keep.append(d)
        return keep

    heads = [0, small]
    bodies = list(range(1, small))

    for cy, cz in zip(heads + bodies, bodies + heads):
        for d in live:
            forward(me, cz if d < 2 else cy, d, None)

    t_copies = []
    for s in range(1, nc):
        t_copies.append(pltpu.make_async_remote_copy(
            src_ref=tbuf.at[col], dst_ref=tbuf.at[col],
            send_sem=t_send.at[s], recv_sem=t_recv.at[s],
            device_id=(me, lax.rem(col + s, nc)), device_id_type=MESH))
        t_copies[-1].start()

    def event(a, b, cs, first):
        valid = inside(-a, -b)
        src = me - a * ny - b
        for c in cs:
            @pl.when(valid)
            def _():
                arrive(src, c)

            for d in step_dirs(a, b, first):
                forward(src, c, d, valid)

    for key in range(1, nz + ny - 1):
        for db in range(0, ny - 1):
            da = key - db
            if da >= nz or da < 0:
                continue
            for c in bodies:
                for a in signs(da):
                    for b in signs(db):
                        event(a, b, [c], False)
        for db in range(min(key, ny - 1), -1, -1):
            da = key - db
            if da >= nz:
                continue
            for a in signs(da):
                for b in signs(db):
                    event(a, b, heads, True)

    for t in t_copies:
        t.wait()

    acc[...] = jnp.zeros_like(acc)
    wide = 2 * tile

    def multiply(src):
        left = tbuf[src // kpc, :rows, pl.ds(pl.multiple_of(lax.rem(src, kpc) * tile, tile), tile)]
        for n in range(0, cap * tile, wide):
            acc[:, n:n + wide] += jnp.dot(left, vbuf[src, :, n:n + wide], preferred_element_type=f32)

    def local(zz, carry):
        multiply(zz * ny + y)
        return carry

    lax.fori_loop(0, nz, local, 0)

    p_ref[...] = jnp.zeros_like(p_ref)
    for i in range(mr):
        best = jnp.zeros((1, posbuf.shape[2]), f32)
        for src in range(nr):
            kk = (src % kpc) * tile
            flag = tbuf[src // kpc, rows:, kk:kk + tile].astype(f32)[i:i + 1]
            best = jnp.maximum(best, flag * posbuf[src, 0:1, :])
        p_ref[i:i + 1, :] = best.astype(jnp.int32)

    for src, c, d, ok in sent[:3 * len(sent) // 4]:
        @pl.when(ok)
        def _():
            copy(src, c, d).wait_send()

    far = [b for b in range(-(ny - 1), ny) if b != 0]

    def across(s, carry):
        dist = (s + 1) // 2
        a = jnp.where(s % 2 == 1, dist, -dist)
        zz = z - a
        for b in far:
            ok = (zz >= 0) & (zz < nz) & (y - b >= 0) & (y - b < ny)
            src = zz * ny + y - b

            @pl.when(ok)
            def _():
                if abs(b) == ny - 1:
                    for c in bodies:
                        arrive(src, c)
                multiply(src)
        return carry

    lax.fori_loop(0, 2 * nz - 1, across, 0)

    for src, c, d, ok in sent[3 * len(sent) // 4:]:
        @pl.when(ok)
        def _():
            copy(src, c, d).wait_send()

    o_ref[...] = acc[...].astype(o_ref.dtype)


def spread_kernel(per, p_vec, o_ref, out_ref, p_ref, sem):
    tile = out_ref.shape[1] // per

    @pl.when(pl.program_id(0) == 0)
    def _():
        one = pltpu.make_async_copy(p_vec, p_ref, sem)
        one.start()
        one.wait()

    for i in range(out_ref.shape[0] // tile):
        here = slice(i * tile, (i + 1) * tile)
        for q in range(per):
            slot = p_ref[i, pl.program_id(0) * per + q]
            at = pl.multiple_of(jnp.maximum(slot - 1, 0) * tile, tile)
            got = o_ref[here, pl.ds(at, tile)]
            out_ref[here, q * tile:(q + 1) * tile] = jnp.where(slot > 0, got, jnp.zeros_like(got))


def solution(mesh):
    nz, ny = grid_of(mesh)
    nc = mesh.shape["col"]

    def on_device(t2_amps, v_ints, t2_mask, v_mask):
        rows, kcols = t2_amps.shape
        tile, ncols = v_ints.shape
        mr = t2_mask.shape[0]
        nt = v_mask.shape[1]
        cap = nt // 2
        nr = nz * ny
        pieces = 6
        vmem = pl.BlockSpec(memory_space=pltpu.VMEM)
        whole = pl.BlockSpec(memory_space=pl.ANY)
        smem = pl.BlockSpec(memory_space=pltpu.SMEM)
        dense, places = pl.pallas_call(
            functools.partial(gather_kernel, nz, ny, nc),
            name="gather",
            out_shape=(pltpu.VMEM((rows, cap * tile), jnp.bfloat16), pltpu.VMEM((8, 128), jnp.int32)),
            in_specs=[smem, smem, whole, whole],
            out_specs=(vmem, vmem),
            scratch_shapes=[
                pltpu.VMEM((rows, kcols), jnp.bfloat16),
                pltpu.VMEM((tile, ncols), jnp.bfloat16),
                pltpu.SemaphoreType.DMA((2,)),
                pltpu.VMEM((nc, rows + 16, kcols), jnp.bfloat16),
                pltpu.VMEM((nr, tile, cap * tile), jnp.bfloat16),
                pltpu.VMEM((nr, 8, 128), jnp.float32),
                pltpu.VMEM((rows, cap * tile), jnp.float32),
                pltpu.SemaphoreType.DMA((nc,)),
                pltpu.SemaphoreType.DMA((nc,)),
                pltpu.SemaphoreType.DMA((4, nr, pieces)),
                pltpu.SemaphoreType.DMA((nr, pieces)),
            ],
            compiler_params=pltpu.CompilerParams(collective_id=0, has_side_effects=True),
        )(t2_mask, v_mask, t2_amps, v_ints)
        dense = pltpu.with_memory_space_constraint(dense, pltpu.VMEM)
        places = pltpu.with_memory_space_constraint(places, pltpu.VMEM)
        per = max(nt // 4, 1)
        return pl.pallas_call(
            functools.partial(spread_kernel, per),
            name="spread",
            grid=(nt // per,),
            out_shape=jax.ShapeDtypeStruct((rows, ncols), jnp.bfloat16),
            in_specs=[vmem, vmem],
            out_specs=pl.BlockSpec((rows, per * tile), lambda n: (0, n)),
            scratch_shapes=[pltpu.SMEM((8, 128), jnp.int32), pltpu.SemaphoreType.DMA],
        )(places, dense)

    return jax.shard_map(
        on_device,
        mesh=mesh,
        in_specs=(P("row", "col"), P("row", "col"), P("row", "col"), P("row", "col")),
        out_specs=P("row", "col"),
        check_vma=False,
    )
```

```python
import functools

import jax
import jax.numpy as jnp
from jax import lax
from jax.experimental import pallas as pl
from jax.experimental.pallas import tpu as pltpu
from jax.sharding import PartitionSpec as P

MESH = pl.DeviceIdType.MESH


def grid_of(mesh):
    rows = mesh.shape["row"]
    ny = 1
    while 2 * (2 * ny) * (2 * ny) <= rows:
        ny *= 2
    return (rows // ny, ny) if rows % ny == 0 else (rows, 1)


def signs(d):
    return (0,) if d == 0 else (d, -d)


def gather_kernel(nz, ny, nc, tm_hbm, vm_hbm, t_hbm, v_hbm, o_ref, p_ref,
                  tm_ref, vm_ref, t_ref, v_ref, p_vec, load, tbuf, vbuf, posbuf, acc, t_send, t_recv, send, recv):
    me, col = lax.axis_index("row"), lax.axis_index("col")
    z, y = me // ny, me % ny
    mr, kpc = tm_ref.shape
    nt = vm_ref.shape[1]
    tile = v_ref.shape[0]
    rows = t_ref.shape[0]
    cap = nt // 2
    nr = nz * ny
    f32 = jnp.float32

    dirs = ((1, 0), (-1, 0), (0, 1), (0, -1))

    def inside(dz, dy):
        ok = jnp.bool_(True)
        if dz > 0:
            ok = ok & (z + dz < nz)
        if dz < 0:
            ok = ok & (z + dz >= 0)
        if dy > 0:
            ok = ok & (y + dy < ny)
        if dy < 0:
            ok = ok & (y + dy >= 0)
        return ok

    live = [d for d in range(4) if (nz > 1 if d < 2 else ny > 1)]

    barrier = pltpu.get_barrier_semaphore()
    expect = jnp.int32(nc - 1)
    for d in live:
        dz, dy = dirs[d]
        ok = inside(dz, dy)
        expect = expect + ok.astype(jnp.int32)

        @pl.when(ok)
        def _():
            pl.semaphore_signal(barrier, inc=1, device_id=(me + dz * ny + dy, col), device_id_type=MESH)

    for s in range(1, nc):
        pl.semaphore_signal(barrier, inc=1, device_id=(me, lax.rem(col + s, nc)), device_id_type=MESH)

    loads = [pltpu.make_async_copy(src, dst, load.at[i]) for i, (src, dst) in enumerate(
        ((vm_hbm, vm_ref), (tm_hbm, tm_ref), (v_hbm, v_ref), (t_hbm, t_ref)))]
    for one in loads:
        one.start()
    for one in loads[:2]:
        one.wait()

    bf16 = jnp.bfloat16
    count, slots = jnp.int32(0), []
    for n in range(nt):
        m = vm_ref[0, n]
        slots.append(jnp.broadcast_to((m * (count + 1)).astype(f32), (16, tile)))
        count = count + m

    def down(x):
        return jnp.broadcast_to(x.astype(bf16)[None], (tile // 16, 16, tile)).reshape(tile, tile)

    for one in loads[2:]:
        one.wait()
    for j in range(cap):
        total = None
        for n in range(j, nt):
            hit = down(jnp.maximum(1.0 - jnp.abs(slots[n] - (j + 1.0)), 0.0))
            term = v_ref[:, n * tile:(n + 1) * tile] * hit
            total = term if total is None else total + term
        vbuf[me, :, j * tile:(j + 1) * tile] = total
    lane = lax.broadcasted_iota(jnp.int32, posbuf.shape[1:], 1)
    place = jnp.zeros(posbuf.shape[1:], f32)
    for n in range(nt):
        place = jnp.where(lane == n, slots[n][:8], place)
    posbuf[me] = place
    for i in range(mr):
        for k in range(kpc):
            part = t_ref[i * tile:(i + 1) * tile, k * tile:(k + 1) * tile]
            flag = down(jnp.broadcast_to(tm_ref[i, k].astype(f32), (16, tile)))
            tbuf[col, i * tile:(i + 1) * tile, k * tile:(k + 1) * tile] = part * flag
    row16 = lax.broadcasted_iota(jnp.int32, (tbuf.shape[1] - rows, tile), 0)
    for k in range(kpc):
        flags = jnp.zeros(row16.shape, f32)
        for i in range(mr):
            flags = jnp.where(row16 == i, tm_ref[i, k].astype(f32), flags)
        tbuf[col, rows:, k * tile:(k + 1) * tile] = flags.astype(tbuf.dtype)

    pl.semaphore_wait(barrier, expect)

    head = tile // 8
    full = cap * tile
    cuts = [(0, head, 0, full), (head, 2 * head, 0, full), (3 * head, 2 * head, 0, full),
            (5 * head, 2 * head, 0, full), (7 * head, head, 0, full)]
    small = len(cuts)

    def piece(src, c):
        if c == small:
            return posbuf.at[src]
        return vbuf.at[src, pl.ds(cuts[c][0], cuts[c][1]), pl.ds(cuts[c][2], cuts[c][3])]

    def copy(src, c, d):
        dz, dy = dirs[d]
        return pltpu.make_async_remote_copy(
            src_ref=piece(src, c), dst_ref=piece(src, c),
            send_sem=send.at[d, src, c], recv_sem=recv.at[src, c],
            device_id=(me + dz * ny + dy, col), device_id_type=MESH)

    sent = []

    def forward(src, c, d, valid):
        dz, dy = dirs[d]
        ok = inside(dz, dy) if valid is None else valid & inside(dz, dy)

        @pl.when(ok)
        def _():
            copy(src, c, d).start()

        sent.append((src, c, d, ok))

    def arrive(src, c):
        pltpu.make_async_remote_copy(
            src_ref=piece(src, c), dst_ref=piece(src, c),
            send_sem=send.at[0, src, c], recv_sem=recv.at[src, c],
            device_id=(me, col), device_id_type=MESH).wait_recv()

    def step_dirs(a, b, first):
        zdir = [0] if a > 0 else [1] if a < 0 else [0, 1]
        ydir = [2] if b > 0 else [3] if b < 0 else [2, 3]
        if first:
            out = zdir + (ydir if a == 0 else [])
        else:
            out = (zdir if b == 0 else []) + ydir
        keep = []
        for d in out:
            if d not in live:
                continue
            if d < 2 and abs(a + dirs[d][0]) >= nz:
                continue
            if d >= 2 and abs(b + dirs[d][1]) >= ny:
                continue
            keep.append(d)
        return keep

    heads = [0, small]
    bodies = list(range(1, small))

    for cy, cz in zip(heads + bodies, bodies + heads):
        for d in live:
            forward(me, cz if d < 2 else cy, d, None)

    t_copies = []
    for s in range(1, nc):
        t_copies.append(pltpu.make_async_remote_copy(
            src_ref=tbuf.at[col], dst_ref=tbuf.at[col],
            send_sem=t_send.at[s], recv_sem=t_recv.at[s],
            device_id=(me, lax.rem(col + s, nc)), device_id_type=MESH))
        t_copies[-1].start()

    def event(a, b, cs, first):
        valid = inside(-a, -b)
        src = me - a * ny - b
        for c in cs:
            @pl.when(valid)
            def _():
                arrive(src, c)

            for d in step_dirs(a, b, first):
                forward(src, c, d, valid)

    for key in range(1, nz + ny - 1):
        for db in range(0, ny - 1):
            da = key - db
            if da >= nz or da < 0:
                continue
            for c in bodies:
                for a in signs(da):
                    for b in signs(db):
                        event(a, b, [c], False)
        for db in range(min(key, ny - 1), -1, -1):
            da = key - db
            if da >= nz:
                continue
            for a in signs(da):
                for b in signs(db):
                    event(a, b, heads, True)

    for t in t_copies:
        t.wait()

    acc[...] = jnp.zeros_like(acc)
    wide = 2 * tile

    def multiply(src):
        left = tbuf[src // kpc, :rows, pl.ds(pl.multiple_of(lax.rem(src, kpc) * tile, tile), tile)]
        for n in range(0, cap * tile, wide):
            acc[:, n:n + wide] += jnp.dot(left, vbuf[src, :, n:n + wide], preferred_element_type=f32)

    def local(zz, carry):
        multiply(zz * ny + y)
        return carry

    lax.fori_loop(0, nz, local, 0)

    p_vec[...] = jnp.zeros_like(p_vec)
    for i in range(mr):
        best = jnp.zeros((1, posbuf.shape[2]), f32)
        for src in range(nr):
            kk = (src % kpc) * tile
            flag = tbuf[src // kpc, rows:, kk:kk + tile].astype(f32)[i:i + 1]
            best = jnp.maximum(best, flag * posbuf[src, 0:1, :])
        p_vec[i:i + 1, :] = best.astype(jnp.int32)

    give = pltpu.make_async_copy(p_vec, p_ref, load.at[4])
    give.start()

    for src, c, d, ok in sent[:3 * len(sent) // 4]:
        @pl.when(ok)
        def _():
            copy(src, c, d).wait_send()

    far = [b for b in range(-(ny - 1), ny) if b != 0]

    def across(s, carry):
        dist = (s + 1) // 2
        a = jnp.where(s % 2 == 1, dist, -dist)
        zz = z - a
        for b in far:
            ok = (zz >= 0) & (zz < nz) & (y - b >= 0) & (y - b < ny)
            src = zz * ny + y - b

            @pl.when(ok)
            def _():
                if abs(b) == ny - 1:
                    for c in bodies:
                        arrive(src, c)
                multiply(src)
        return carry

    lax.fori_loop(0, 2 * nz - 1, across, 0)

    for src, c, d, ok in sent[3 * len(sent) // 4:]:
        @pl.when(ok)
        def _():
            copy(src, c, d).wait_send()

    give.wait()
    o_ref[...] = acc[...].astype(o_ref.dtype)


def spread_kernel(per, p_ref, o_ref, out_ref):
    tile = out_ref.shape[1] // per

    for i in range(out_ref.shape[0] // tile):
        here = slice(i * tile, (i + 1) * tile)
        for q in range(per):
            slot = p_ref[i, pl.program_id(0) * per + q]
            at = pl.multiple_of(jnp.maximum(slot - 1, 0) * tile, tile)
            got = o_ref[here, pl.ds(at, tile)]
            out_ref[here, q * tile:(q + 1) * tile] = jnp.where(slot > 0, got, jnp.zeros_like(got))


def solution(mesh):
    nz, ny = grid_of(mesh)
    nc = mesh.shape["col"]

    def on_device(t2_amps, v_ints, t2_mask, v_mask):
        rows, kcols = t2_amps.shape
        tile, ncols = v_ints.shape
        mr = t2_mask.shape[0]
        nt = v_mask.shape[1]
        cap = nt // 2
        nr = nz * ny
        pieces = 6
        vmem = pl.BlockSpec(memory_space=pltpu.VMEM)
        whole = pl.BlockSpec(memory_space=pl.ANY)
        smem = pl.BlockSpec(memory_space=pltpu.SMEM)
        dense, places = pl.pallas_call(
            functools.partial(gather_kernel, nz, ny, nc),
            name="gather",
            out_shape=(pltpu.VMEM((rows, cap * tile), jnp.bfloat16), pltpu.SMEM((8, 128), jnp.int32)),
            in_specs=[whole] * 4,
            out_specs=(vmem, smem),
            scratch_shapes=[
                pltpu.SMEM(t2_mask.shape, jnp.int32),
                pltpu.SMEM(v_mask.shape, jnp.int32),
                pltpu.VMEM((rows, kcols), jnp.bfloat16),
                pltpu.VMEM((tile, ncols), jnp.bfloat16),
                pltpu.VMEM((8, 128), jnp.int32),
                pltpu.SemaphoreType.DMA((5,)),
                pltpu.VMEM((nc, rows + 16, kcols), jnp.bfloat16),
                pltpu.VMEM((nr, tile, cap * tile), jnp.bfloat16),
                pltpu.VMEM((nr, 8, 128), jnp.float32),
                pltpu.VMEM((rows, cap * tile), jnp.float32),
                pltpu.SemaphoreType.DMA((nc,)),
                pltpu.SemaphoreType.DMA((nc,)),
                pltpu.SemaphoreType.DMA((4, nr, pieces)),
                pltpu.SemaphoreType.DMA((nr, pieces)),
            ],
            compiler_params=pltpu.CompilerParams(collective_id=0, has_side_effects=True),
        )(t2_mask, v_mask, t2_amps, v_ints)
        dense = pltpu.with_memory_space_constraint(dense, pltpu.VMEM)
        places = pltpu.with_memory_space_constraint(places, pltpu.SMEM)
        per = max(nt // 4, 1)
        return pl.pallas_call(
            functools.partial(spread_kernel, per),
            name="spread",
            grid=(nt // per,),
            out_shape=jax.ShapeDtypeStruct((rows, ncols), jnp.bfloat16),
            in_specs=[smem, vmem],
            out_specs=pl.BlockSpec((rows, per * tile), lambda n: (0, n)),
        )(places, dense)

    return jax.shard_map(
        on_device,
        mesh=mesh,
        in_specs=(P("row", "col"), P("row", "col"), P("row", "col"), P("row", "col")),
        out_specs=P("row", "col"),
        check_vma=False,
    )
```
